32 devices in a mesh: dp: 8 (over z, y), mp: 4 (over x, core).
Axes of the slice: x: 2, y: 2, z: 4, core: 2. Of those that a mesh axis runs over, the one named last changes fastest.
Arguments:
- slow_weights: float32 [1, 3584, 1024], P(None, None, 'mp'), may hold values from -6 to 6
- fast_weights: bfloat16 [8, 1, 3584, 1024], P('dp', None, None, 'mp'), may hold values from -64 to 64
- momentum: float32 [1, 3584, 1024], P(None, None, 'mp'), may hold values from -1.2 to 1.2
Outputs:
- slow_next: float32 [1, 3584, 1024], P(None, None, 'mp')
- momentum_next: float32 [1, 3584, 1024], P(None, None, 'mp')
- fast_next: bfloat16 [8, 1, 3584, 1024], P('dp', None, None, 'mp')
The draws below stay inside these ranges and needn't reach their ends.
All inputs are finite; a program needn't handle non-finite values.
Results may differ from the reference program's by a relative error of at most 0.001.
Values sent between devices are 32-bit elements; how exact they have to be, the bound alone decides.
A program may use at most 64 MiB of HBM per device.

```python
import math
import jax
import jax.numpy as jnp
from jax import lax

D = 3584
LAYERS = 1
KV2 = 1024
REPLICAS = 8


def slow_base(key):
    values = jax.random.normal(jax.random.fold_in(key, 11), (LAYERS, D, KV2), jnp.float32)
    return jnp.clip(values, -6.0, 6.0)


def draw_slow_weights(key, part):
    return slow_base(key)


def draw_fast_weights(key, part):
    slow_values = slow_base(key)
    row_place = jnp.arange(D, dtype=jnp.float32) / D
    col_place = jnp.arange(KV2, dtype=jnp.float32) / KV2
    row_spread = 10.0 ** jax.random.uniform(jax.random.fold_in(key, 12), (D,), jnp.float32)
    col_spread = 10.0 ** jax.random.uniform(jax.random.fold_in(key, 13), (KV2,), jnp.float32)
    common = jax.random.normal(jax.random.fold_in(key, 14), (LAYERS, D, KV2), jnp.float32)
    single = jax.random.normal(jax.random.fold_in(key, 15), (REPLICAS, LAYERS, D, KV2), jnp.float32)
    row_scale = (1.0 + 2.0 * row_place) * row_spread
    col_scale = (1.0 + 2.0 * col_place) * col_spread
    drift = 0.02 * (common[None] + 1.5 * single)
    drift = drift * row_scale[:, None] * col_scale[None, :]
    fast_values = jnp.clip(slow_values[None] - drift, -64.0, 64.0)
    return fast_values.astype(jnp.bfloat16)


def shard_levels(rng, extent, cuts, least, high):
    factor_of = 1.0
    for axis_at, shards_of in cuts:
        heights = jax.random.uniform(jax.random.fold_in(jax.random.fold_in(rng, 6), axis_at), (shards_of,), jnp.float32, least / len(cuts), high / len(cuts))
        factor_of = factor_of * jnp.repeat(jnp.exp(heights), extent[axis_at] // shards_of).reshape((-1,) + (1,) * (len(extent) - 1 - axis_at))
    return factor_of


def gaussian(own_key, dims, deviation, reach, pieces=(), kind=jnp.bfloat16):
    result = jax.random.normal(own_key, dims, jnp.float32) * deviation
    if len(pieces) > 0:
        result = shard_levels(own_key, dims, pieces, -0.22, 0.18) * result
    return jnp.clip(result, min=-reach, max=reach).astype(kind)


def setup_inputs(seed: int = 0) -> dict:
    splits = jax.random.split(jax.random.key(seed), 4)
    return {
        "slow_weights": draw_slow_weights(jax.random.fold_in(splits[3], 71), 0),
        "fast_weights": draw_fast_weights(jax.random.fold_in(splits[3], 71), 0),
        "momentum": gaussian(splits[2], (LAYERS, D, KV2), 0.2, 1.2, ((2, 4),), jnp.float32),
    }


MOMENTUM_RATE = 0.9
OUTER_RATE = 0.7
CLIP_LEVEL = 0.2
EPSILON = 1e-06

def reference(slow_weights, fast_weights, momentum):

    def accumulate(summed, fast_one):
        return (summed + (slow_weights - fast_one.astype(jnp.float32)), None)
    summed, unused = lax.scan(accumulate, jnp.zeros_like(slow_weights), fast_weights)
    pseudo = summed / REPLICAS
    norm_value = jnp.sqrt(jnp.sum(pseudo * pseudo))
    max_norm = CLIP_LEVEL * math.sqrt(LAYERS * D * KV2)
    factor = jnp.minimum(1.0, max_norm / (norm_value + EPSILON))
    gradient = factor * pseudo
    momentum_next = MOMENTUM_RATE * momentum + gradient
    slow_next = slow_weights - OUTER_RATE * (gradient + MOMENTUM_RATE * momentum_next)
    fast_next = jnp.broadcast_to(slow_next.astype(jnp.bfloat16)[None], fast_weights.shape)
    return (slow_next, momentum_next, fast_next)
```

```python
import functools
import math

import jax
import jax.numpy as jnp
from jax import lax
from jax.experimental import pallas as pl
from jax.experimental.pallas import tpu as pltpu
from jax.sharding import PartitionSpec as P

MOMENTUM_RATE = 0.9
OUTER_RATE = 0.7
CLIP_LEVEL = 0.2
EPSILON = 1e-06
MESH = pl.DeviceIdType.MESH
SUBS = 4


def device_at(place, n):
    half = n // 2
    up = 2 * place
    down = 2 * (n - 1 - place) + 1
    return jnp.where(place < half, up, down)


def kernel(n, m, subs, max_norm, slow_ref, fast_ref, pseudo_ref, factor_ref,
           ring, squares, norms, send_sem, recv_sem, norm_send, norm_recv):
    rows, cols = slow_ref.shape
    chunk = rows // n
    sub = chunk // subs
    half = cols // 2
    me = lax.axis_index("dp")
    mine = lax.axis_index("mp")
    z, y = me // 2, lax.rem(me, 2)
    place = jnp.where(y == 0, z, n - 1 - z)
    right = device_at(lax.rem(place + 1, n), n)
    left = device_at(lax.rem(place + n - 1, n), n)
    goal = (right, left)
    order = (place, lax.rem(n - place, n))

    barrier = pltpu.get_barrier_semaphore()
    for other in (left, right):
        pl.semaphore_signal(barrier, inc=1, device_id={"dp": other}, device_id_type=MESH)
    for k in range(1, m):
        pl.semaphore_signal(
            barrier, inc=1, device_id={"mp": lax.rem(mine + k, m)}, device_id_type=MESH
        )

    def start_row(c, b):
        return pl.multiple_of(c * chunk + b * sub, sub)

    def own(d, b, c):
        at = (pl.ds(start_row(c, b), sub), pl.ds(d * half, half))
        return slow_ref[at] - fast_ref[at].astype(jnp.float32)

    def reduce_copy(d, b, s):
        return pltpu.make_async_remote_copy(
            src_ref=ring.at[d, b, s], dst_ref=ring.at[d, b, s + 1],
            send_sem=send_sem.at[d, b, s], recv_sem=recv_sem.at[d, b, s],
            device_id={"dp": goal[d]}, device_id_type=MESH,
        )

    def gather_copy(d, b, s, c):
        at = (pl.ds(start_row(c, b), sub), pl.ds(d * half, half))
        return pltpu.make_async_remote_copy(
            src_ref=pseudo_ref.at[at], dst_ref=pseudo_ref.at[at],
            send_sem=send_sem.at[d, b, n - 1 + s], recv_sem=recv_sem.at[d, b, n - 1 + s],
            device_id={"dp": goal[d]}, device_id_type=MESH,
        )

    def add_squares(d, b, c, value):
        sq = value * value
        squares[d, b, c] = jnp.sum(sq.reshape(sub // 8, 8, half), axis=0)

    streams = [(d, b) for b in range(subs) for d in range(2)]
    for d, b in streams:
        ring[d, b, 0] = own(d, b, order[d])
    pl.semaphore_wait(barrier, 2 + m - 1)
    for d, b in streams:
        reduce_copy(d, b, 0).start()

    def reduce_step(s, carry):
        for d, b in streams:
            reduce_copy(d, b, s).wait_recv()
            c = lax.rem(order[d] - s - 1 + n, n)
            ring[d, b, s + 1] = ring[d, b, s + 1] + own(d, b, c)
            reduce_copy(d, b, s + 1).start()
        return carry

    lax.fori_loop(0, n - 2, reduce_step, 0)
    for d, b in streams:
        reduce_copy(d, b, n - 2).wait_recv()
        c = lax.rem(order[d] + 1, n)
        value = (ring[d, b, n - 1] + own(d, b, c)) / n
        pseudo_ref[pl.ds(start_row(c, b), sub), pl.ds(d * half, half)] = value
        gather_copy(d, b, 0, c).start()
        add_squares(d, b, c, value)

    def gather_step(s, carry):
        for d, b in streams:
            c = lax.rem(order[d] - s + n, n)
            gather_copy(d, b, s, c).wait_recv()
            gather_copy(d, b, s + 1, c).start()
            at = (pl.ds(start_row(c, b), sub), pl.ds(d * half, half))
            add_squares(d, b, c, pseudo_ref[at])
        return carry

    lax.fori_loop(0, n - 2, gather_step, 0)
    for d, b in streams:
        c = lax.rem(order[d] + 2, n)
        gather_copy(d, b, n - 2, c).wait_recv()
        at = (pl.ds(start_row(c, b), sub), pl.ds(d * half, half))
        add_squares(d, b, c, pseudo_ref[at])

    part = jnp.sum(squares[...].reshape(2 * subs * n, 8, half), axis=0)
    norms[mine] = part

    def norm_copy(k):
        return pltpu.make_async_remote_copy(
            src_ref=norms.at[mine], dst_ref=norms.at[mine],
            send_sem=norm_send.at[k], recv_sem=norm_recv.at[k],
            device_id={"mp": lax.rem(mine + k, m)}, device_id_type=MESH,
        )

    for k in range(1, m):
        norm_copy(k).start()

    def drain(s, carry):
        for d, b in streams:
            reduce_copy(d, b, s).wait_send()
            gather_copy(d, b, s, 0).wait_send()
        return carry

    lax.fori_loop(0, n - 1, drain, 0)
    for k in range(1, m):
        norm_copy(k).wait_recv()
    total = norms[0]
    for j in range(1, m):
        total = total + norms[j]
    total = jnp.sum(jnp.sum(total, axis=1, keepdims=True), axis=0, keepdims=True)
    factor = jnp.minimum(1.0, max_norm / (jnp.sqrt(total) + EPSILON))
    factor_ref[...] = jnp.broadcast_to(factor, factor_ref.shape)
    for k in range(1, m):
        norm_copy(k).wait_send()


def body(slow_weights, fast_weights, momentum):
    n, m = lax.axis_size("dp"), lax.axis_size("mp")
    layers, depth, cols = slow_weights.shape
    rows = layers * depth
    max_norm = CLIP_LEVEL * math.sqrt(rows * cols * m)
    subs = SUBS
    while rows % (n * subs * 16):
        subs -= 1
    sub = rows // (n * subs)
    slow = slow_weights.reshape(rows, cols)
    vmem = pl.BlockSpec(memory_space=pltpu.VMEM)
    pseudo, factor = pl.pallas_call(
        functools.partial(kernel, n, m, subs, max_norm),
        out_shape=(
            jax.ShapeDtypeStruct((rows, cols), jnp.float32),
            jax.ShapeDtypeStruct((8, 128), jnp.float32),
        ),
        in_specs=[vmem, vmem],
        out_specs=(vmem, vmem),
        scratch_shapes=[
            pltpu.VMEM((2, subs, n, sub, cols // 2), jnp.float32),
            pltpu.VMEM((2, subs, n, 8, cols // 2), jnp.float32),
            pltpu.VMEM((m, 8, cols // 2), jnp.float32),
            pltpu.SemaphoreType.DMA((2, subs, 2 * n - 2)),
            pltpu.SemaphoreType.DMA((2, subs, 2 * n - 2)),
            pltpu.SemaphoreType.DMA((m,)),
            pltpu.SemaphoreType.DMA((m,)),
        ],
        compiler_params=pltpu.CompilerParams(collective_id=0, has_side_effects=True),
        name="ring",
    )(slow, fast_weights.reshape(rows, cols))
    gradient = factor[0, 0] * pseudo
    momentum_next = MOMENTUM_RATE * momentum.reshape(rows, cols) + gradient
    slow_next = slow - OUTER_RATE * (gradient + MOMENTUM_RATE * momentum_next)
    fast_next = slow_next.astype(jnp.bfloat16).reshape(fast_weights.shape)
    return (
        slow_next.reshape(slow_weights.shape),
        momentum_next.reshape(slow_weights.shape),
        fast_next,
    )


def solution(mesh):
    in_specs = (P(None, None, "mp"), P("dp", None, None, "mp"), P(None, None, "mp"))
    out_specs = (P(None, None, "mp"), P(None, None, "mp"), P("dp", None, None, "mp"))
    return jax.shard_map(body, mesh=mesh, in_specs=in_specs, out_specs=out_specs, check_vma=False)
```

```python
import functools
import math

import jax
import jax.numpy as jnp
from jax import lax
from jax.experimental import pallas as pl
from jax.experimental.pallas import tpu as pltpu
from jax.sharding import PartitionSpec as P

MOMENTUM_RATE = 0.9
OUTER_RATE = 0.7
CLIP_LEVEL = 0.2
EPSILON = 1e-06
MESH = pl.DeviceIdType.MESH
SUBS = 4
VMEM_LIMIT = 24 * 1024 * 1024


def device_at(place, n):
    half = n // 2
    up = 2 * place
    down = 2 * (n - 1 - place) + 1
    return jnp.where(place < half, up, down)


def kernel(n, m, subs, max_norm, slow_hbm, fast_hbm, moment_hbm,
           slow_out, moment_out, fast_out,
           ring, slow_ref, fast_ref, moment_ref, pseudo_ref, parts, norms, moment_sem, load_sem, send_sem, recv_sem,
           part_send, part_recv, norm_send, norm_recv):
    rows, cols = slow_ref.shape
    chunk = rows // n
    sub = chunk // subs
    half = cols // 2
    me = lax.axis_index("dp")
    mine = lax.axis_index("mp")
    z, y = me // 2, lax.rem(me, 2)
    place = jnp.where(y == 0, z, n - 1 - z)
    right = device_at(lax.rem(place + 1, n), n)
    left = device_at(lax.rem(place + n - 1, n), n)
    goal = (right, left)
    order = (place, lax.rem(n - place, n))

    def load(d, k):
        c = lax.rem(order[d] - k + n, n)
        at = (pl.ds(pl.multiple_of(c * chunk, chunk), chunk), pl.ds(d * half, half))
        return (
            pltpu.make_async_copy(slow_hbm.at[at], slow_ref.at[at], load_sem.at[0, d, k]),
            pltpu.make_async_copy(fast_hbm.at[at], fast_ref.at[at], load_sem.at[1, d, k]),
        )

    for d in range(2):
        for copy in load(d, 0):
            copy.start()
    barrier = pltpu.get_barrier_semaphore()
    for k in range(1, n):
        pl.semaphore_signal(
            barrier, inc=1, device_id={"dp": lax.rem(me + k, n)}, device_id_type=MESH
        )
    for k in range(1, m):
        pl.semaphore_signal(
            barrier, inc=1, device_id={"mp": lax.rem(mine + k, m)}, device_id_type=MESH
        )
    moment_load = pltpu.make_async_copy(moment_hbm, moment_ref, moment_sem)

    def start_row(c, b):
        return pl.multiple_of(c * chunk + b * sub, sub)

    def own(d, b, c):
        at = (pl.ds(start_row(c, b), sub), pl.ds(d * half, half))
        return slow_ref[at] - fast_ref[at].astype(jnp.float32)

    def reduce_copy(d, b, s):
        return pltpu.make_async_remote_copy(
            src_ref=ring.at[d, b, s], dst_ref=ring.at[d, b, s + 1],
            send_sem=send_sem.at[d, b, s], recv_sem=recv_sem.at[d, b, s],
            device_id={"dp": goal[d]}, device_id_type=MESH,
        )

    def gather_copy(d, b, s, c):
        at = (pl.ds(start_row(c, b), sub), pl.ds(d * half, half))
        return pltpu.make_async_remote_copy(
            src_ref=pseudo_ref.at[at], dst_ref=pseudo_ref.at[at],
            send_sem=send_sem.at[d, b, n - 1 + s], recv_sem=recv_sem.at[d, b, n - 1 + s],
            device_id={"dp": goal[d]}, device_id_type=MESH,
        )

    def part_copy(k):
        return pltpu.make_async_remote_copy(
            src_ref=parts.at[me], dst_ref=parts.at[me],
            send_sem=part_send.at[k], recv_sem=part_recv.at[k],
            device_id={"dp": lax.rem(me + k, n)}, device_id_type=MESH,
        )

    def norm_copy(k):
        return pltpu.make_async_remote_copy(
            src_ref=norms.at[mine], dst_ref=norms.at[mine],
            send_sem=norm_send.at[k], recv_sem=norm_recv.at[k],
            device_id={"mp": lax.rem(mine + k, m)}, device_id_type=MESH,
        )

    streams = [(d, b) for b in range(subs) for d in range(2)]
    for d in range(2):
        for copy in load(d, 0):
            copy.wait()
    for d, b in streams:
        ring[d, b, 0] = own(d, b, order[d])
    pl.semaphore_wait(barrier, n - 1 + m - 1)
    for d, b in streams:
        reduce_copy(d, b, 0).start()
    for k in range(1, n):
        for d in range(2):
            for copy in load(d, k):
                copy.start()
    moment_load.start()

    def reduce_step(s, carry):
        for d in range(2):
            for copy in load(d, s + 1):
                copy.wait()
        for d, b in streams:
            c = lax.rem(order[d] - s - 1 + n, n)
            reduce_copy(d, b, s).wait_recv()
            ring[d, b, s + 1] = ring[d, b, s + 1] + own(d, b, c)
            reduce_copy(d, b, s + 1).start()
        return carry

    lax.fori_loop(0, n - 2, reduce_step, 0)
    for d in range(2):
        for copy in load(d, n - 1):
            copy.wait()
    part = jnp.zeros((8, half), jnp.float32)
    for d, b in streams:
        c = lax.rem(order[d] + 1, n)
        reduce_copy(d, b, n - 2).wait_recv()
        value = (ring[d, b, n - 1] + own(d, b, c)) / n
        pseudo_ref[pl.ds(start_row(c, b), sub), pl.ds(d * half, half)] = value
        gather_copy(d, b, 0, c).start()
        part = part + jnp.sum((value * value).reshape(sub // 8, 8, half), axis=0)
    parts[me] = part

    def gather_step(s, carry):
        for d, b in streams:
            c = lax.rem(order[d] - s + n, n)
            gather_copy(d, b, s, c).wait_recv()
            gather_copy(d, b, s + 1, c).start()
        return carry

    second = (n - 2) // 2
    first = second // 2
    for k in range(1, n):
        part_copy(k).start()
    lax.fori_loop(0, first, gather_step, 0)
    for k in range(1, n):
        part_copy(k).wait_recv()
    norm = parts[0]
    for j in range(1, n):
        norm = norm + parts[j]
    norms[mine] = norm
    for k in range(1, m):
        norm_copy(k).start()
    lax.fori_loop(first, second, gather_step, 0)
    for k in range(1, m):
        norm_copy(k).wait_recv()
    total = norms[0]
    for j in range(1, m):
        total = total + norms[j]
    total = jnp.sum(jnp.sum(total, axis=1, keepdims=True), axis=0, keepdims=True)
    factor = jnp.minimum(1.0, max_norm / (jnp.sqrt(total) + EPSILON))
    moment_load.wait()

    def update(d, c):
        at = (pl.ds(pl.multiple_of(c * chunk, chunk), chunk), pl.ds(d * half, half))
        gradient = factor * pseudo_ref[at]
        moment = MOMENTUM_RATE * moment_ref[at] + gradient
        slow = slow_ref[at] - OUTER_RATE * (gradient + MOMENTUM_RATE * moment)
        moment_out[at] = moment
        slow_out[at] = slow
        fast_out[at] = slow.astype(fast_out.dtype)

    def update_step(s, carry):
        gather_step(s, carry)
        for d in range(2):
            update(d, lax.rem(order[d] - s + n, n))
            update(d, lax.rem(order[d] - (s - second) + n, n))
        return carry

    lax.fori_loop(second, n - 2, update_step, 0)
    for d in range(2):
        update(d, lax.rem(order[d] + 1, n))
    for k in range(1, n):
        part_copy(k).wait_send()
    for k in range(1, m):
        norm_copy(k).wait_send()

    def drain(s, carry):
        for d, b in streams:
            reduce_copy(d, b, s).wait_send()
            gather_copy(d, b, s, 0).wait_send()
        return carry

    lax.fori_loop(0, n - 2, drain, 0)
    for d, b in streams:
        c = lax.rem(order[d] + 2, n)
        reduce_copy(d, b, n - 2).wait_send()
        gather_copy(d, b, n - 2, c).wait()
    for d in range(2):
        update(d, lax.rem(order[d] + 2, n))


def emit_kernel(pieces, *refs):
    count = len(refs) // 2
    sources, targets, sem = refs[:count], refs[count:-1], refs[-1]
    size = sources[0].shape[0] // pieces
    copies = [
        pltpu.make_async_copy(
            sources[i].at[pl.ds(k * size, size)], targets[i].at[pl.ds(k * size, size)], sem.at[i, k]
        )
        for k in range(pieces) for i in range(count)
    ]
    for copy in copies:
        copy.start()
    for copy in copies:
        copy.wait()


def emit(arrays, pieces):
    return pl.pallas_call(
        functools.partial(emit_kernel, pieces),
        out_shape=tuple(jax.ShapeDtypeStruct(x.shape, x.dtype) for x in arrays),
        in_specs=[pl.BlockSpec(memory_space=pltpu.VMEM)] * len(arrays),
        out_specs=tuple(pl.BlockSpec(memory_space=pltpu.HBM) for _ in arrays),
        scratch_shapes=[pltpu.SemaphoreType.DMA((len(arrays), pieces))],
        compiler_params=pltpu.CompilerParams(vmem_limit_bytes=VMEM_LIMIT),
        name="emit",
    )(*arrays)


def body(slow_weights, fast_weights, momentum):
    n, m = lax.axis_size("dp"), lax.axis_size("mp")
    layers, depth, cols = slow_weights.shape
    rows = layers * depth
    max_norm = CLIP_LEVEL * math.sqrt(rows * cols * m)
    subs = SUBS
    while rows % (n * subs * 16):
        subs -= 1
    sub = rows // (n * subs)
    slow = slow_weights.reshape(rows, cols)
    hbm = pl.BlockSpec(memory_space=pltpu.HBM)
    vmem = pl.BlockSpec(memory_space=pltpu.VMEM)
    flat = (slow_weights, fast_weights, momentum)
    flat = [
        pltpu.with_memory_space_constraint(x.reshape(rows, cols), pltpu.HBM) for x in flat
    ]
    results = pl.pallas_call(
        functools.partial(kernel, n, m, subs, max_norm),
        out_shape=(
            jax.ShapeDtypeStruct((rows, cols), jnp.float32),
            jax.ShapeDtypeStruct((rows, cols), jnp.float32),
            jax.ShapeDtypeStruct((rows, cols), jnp.bfloat16),
        ),
        in_specs=[hbm, hbm, hbm],
        out_specs=(vmem, vmem, vmem),
        scratch_shapes=[
            pltpu.VMEM((2, subs, n, sub, cols // 2), jnp.float32),
            pltpu.VMEM((rows, cols), jnp.float32),
            pltpu.VMEM((rows, cols), jnp.bfloat16),
            pltpu.VMEM((rows, cols), jnp.float32),
            pltpu.VMEM((rows, cols), jnp.float32),
            pltpu.VMEM((n, 8, cols // 2), jnp.float32),
            pltpu.VMEM((m, 8, cols // 2), jnp.float32),
            pltpu.SemaphoreType.DMA,
            pltpu.SemaphoreType.DMA((2, 2, n)),
            pltpu.SemaphoreType.DMA((2, subs, 2 * n - 2)),
            pltpu.SemaphoreType.DMA((2, subs, 2 * n - 2)),
            pltpu.SemaphoreType.DMA((n,)),
            pltpu.SemaphoreType.DMA((n,)),
            pltpu.SemaphoreType.DMA((m,)),
            pltpu.SemaphoreType.DMA((m,)),
        ],
        compiler_params=pltpu.CompilerParams(
            collective_id=0, has_side_effects=True, vmem_limit_bytes=VMEM_LIMIT
        ),
        name="ring",
    )(*flat)
    slow_next, momentum_next, fast_next = emit(results, 4)
    return (
        slow_next.reshape(slow_weights.shape),
        momentum_next.reshape(slow_weights.shape),
        fast_next.reshape(fast_weights.shape),
    )


def solution(mesh):
    in_specs = (P(None, None, "mp"), P("dp", None, None, "mp"), P(None, None, "mp"))
    out_specs = (P(None, None, "mp"), P(None, None, "mp"), P("dp", None, None, "mp"))
    return jax.shard_map(body, mesh=mesh, in_specs=in_specs, out_specs=out_specs, check_vma=False)
```

```python
import functools
import math

import jax
import jax.numpy as jnp
from jax import lax
from jax.experimental import pallas as pl
from jax.experimental.pallas import tpu as pltpu
from jax.sharding import PartitionSpec as P

MOMENTUM_RATE = 0.9
OUTER_RATE = 0.7
CLIP_LEVEL = 0.2
EPSILON = 1e-06
MESH = pl.DeviceIdType.MESH
SUBS = 4
VMEM_LIMIT = 24 * 1024 * 1024


def device_at(place, n):
    half = n // 2
    up = 2 * place
    down = 2 * (n - 1 - place) + 1
    return jnp.where(place < half, up, down)


def kernel(n, m, subs, max_norm, slow_hbm, fast_hbm, moment_hbm,
           slow_out, moment_out, fast_out,
           ring, slow_ref, fast_ref, moment_ref, pseudo_ref, parts, norms, moment_sem, load_sem, send_sem, recv_sem,
           part_send, part_recv, norm_send, norm_recv):
    rows, cols = slow_ref.shape
    chunk = rows // n
    sub = chunk // subs
    half = cols // 2
    me = lax.axis_index("dp")
    mine = lax.axis_index("mp")
    z, y = me // 2, lax.rem(me, 2)
    place = jnp.where(y == 0, z, n - 1 - z)
    right = device_at(lax.rem(place + 1, n), n)
    left = device_at(lax.rem(place + n - 1, n), n)
    goal = (right, left)
    order = (place, lax.rem(n - place, n))

    def load(d, k):
        c = lax.rem(order[d] - k + n, n)
        at = (pl.ds(pl.multiple_of(c * chunk, chunk), chunk), pl.ds(d * half, half))
        return (
            pltpu.make_async_copy(slow_hbm.at[at], slow_ref.at[at], load_sem.at[0, d, k]),
            pltpu.make_async_copy(fast_hbm.at[at], fast_ref.at[at], load_sem.at[1, d, k]),
        )

    for d in range(2):
        for copy in load(d, 0):
            copy.start()
    barrier = pltpu.get_barrier_semaphore()
    for other in (left, right):
        pl.semaphore_signal(barrier, inc=1, device_id={"dp": other}, device_id_type=MESH)
    for k in range(1, m):
        pl.semaphore_signal(
            barrier, inc=1, device_id={"mp": lax.rem(mine + k, m)}, device_id_type=MESH
        )
    moment_load = pltpu.make_async_copy(moment_hbm, moment_ref, moment_sem)

    def start_row(c, b):
        return pl.multiple_of(c * chunk + b * sub, sub)

    def own(d, b, c):
        at = (pl.ds(start_row(c, b), sub), pl.ds(d * half, half))
        return slow_ref[at] - fast_ref[at].astype(jnp.float32)

    def reduce_copy(d, b, s):
        return pltpu.make_async_remote_copy(
            src_ref=ring.at[d, b, s], dst_ref=ring.at[d, b, s + 1],
            send_sem=send_sem.at[d, b, s], recv_sem=recv_sem.at[d, b, s],
            device_id={"dp": goal[d]}, device_id_type=MESH,
        )

    def gather_copy(d, b, s, c):
        at = (pl.ds(start_row(c, b), sub), pl.ds(d * half, half))
        return pltpu.make_async_remote_copy(
            src_ref=pseudo_ref.at[at], dst_ref=pseudo_ref.at[at],
            send_sem=send_sem.at[d, b, n - 1 + s], recv_sem=recv_sem.at[d, b, n - 1 + s],
            device_id={"dp": goal[d]}, device_id_type=MESH,
        )

    def part_copy(k):
        return pltpu.make_async_remote_copy(
            src_ref=parts.at[me], dst_ref=parts.at[me],
            send_sem=part_send.at[k], recv_sem=part_recv.at[k],
            device_id={"dp": lax.rem(me + k, n)}, device_id_type=MESH,
        )

    def norm_copy(k):
        return pltpu.make_async_remote_copy(
            src_ref=norms.at[mine], dst_ref=norms.at[mine],
            send_sem=norm_send.at[k], recv_sem=norm_recv.at[k],
            device_id={"mp": lax.rem(mine + k, m)}, device_id_type=MESH,
        )

    streams = [(d, b) for b in range(subs) for d in range(2)]
    for d in range(2):
        for copy in load(d, 0):
            copy.wait()
    for d, b in streams:
        ring[d, b, 0] = own(d, b, order[d])
    pl.semaphore_wait(barrier, 2 + m - 1)
    for d, b in streams:
        reduce_copy(d, b, 0).start()
    for k in range(1, n):
        for d in range(2):
            for copy in load(d, k):
                copy.start()
    moment_load.start()

    def reduce_step(s, carry):
        for d in range(2):
            for copy in load(d, s + 1):
                copy.wait()
        for d, b in streams:
            c = lax.rem(order[d] - s - 1 + n, n)
            reduce_copy(d, b, s).wait_recv()
            ring[d, b, s + 1] = ring[d, b, s + 1] + own(d, b, c)
            reduce_copy(d, b, s + 1).start()
        return carry

    lax.fori_loop(0, n - 2, reduce_step, 0)
    for d in range(2):
        for copy in load(d, n - 1):
            copy.wait()
    part = jnp.zeros((8, half), jnp.float32)
    for d, b in streams:
        c = lax.rem(order[d] + 1, n)
        reduce_copy(d, b, n - 2).wait_recv()
        value = (ring[d, b, n - 1] + own(d, b, c)) / n
        pseudo_ref[pl.ds(start_row(c, b), sub), pl.ds(d * half, half)] = value
        gather_copy(d, b, 0, c).start()
        part = part + jnp.sum((value * value).reshape(sub // 8, 8, half), axis=0)
    parts[me] = part

    def gather_step(s, carry):
        for d, b in streams:
            c = lax.rem(order[d] - s + n, n)
            gather_copy(d, b, s, c).wait_recv()
            gather_copy(d, b, s + 1, c).start()
        return carry

    second = (n - 2) // 2
    first = second // 2
    for k in range(1, n):
        part_copy(k).start()
    lax.fori_loop(0, first, gather_step, 0)
    for k in range(1, n):
        part_copy(k).wait_recv()
    norm = parts[0]
    for j in range(1, n):
        norm = norm + parts[j]
    norms[mine] = norm
    for k in range(1, m):
        norm_copy(k).start()
    lax.fori_loop(first, second, gather_step, 0)
    for k in range(1, m):
        norm_copy(k).wait_recv()
    total = norms[0]
    for j in range(1, m):
        total = total + norms[j]
    total = jnp.sum(jnp.sum(total, axis=1, keepdims=True), axis=0, keepdims=True)
    factor = jnp.minimum(1.0, max_norm / (jnp.sqrt(total) + EPSILON))
    moment_load.wait()

    def update(d, c):
        at = (pl.ds(pl.multiple_of(c * chunk, chunk), chunk), pl.ds(d * half, half))
        gradient = factor * pseudo_ref[at]
        moment = MOMENTUM_RATE * moment_ref[at] + gradient
        slow = slow_ref[at] - OUTER_RATE * (gradient + MOMENTUM_RATE * moment)
        moment_out[at] = moment
        slow_out[at] = slow
        fast_out[at] = slow.astype(fast_out.dtype)

    def update_step(s, carry):
        gather_step(s, carry)
        for d in range(2):
            update(d, lax.rem(order[d] - s + n, n))
            update(d, lax.rem(order[d] - (s - second) + n, n))
        return carry

    lax.fori_loop(second, n - 2, update_step, 0)
    for d in range(2):
        update(d, lax.rem(order[d] + 1, n))
    for k in range(1, n):
        part_copy(k).wait_send()
    for k in range(1, m):
        norm_copy(k).wait_send()

    def drain(s, carry):
        for d, b in streams:
            reduce_copy(d, b, s).wait_send()
            gather_copy(d, b, s, 0).wait_send()
        return carry

    lax.fori_loop(0, n - 2, drain, 0)
    for d, b in streams:
        c = lax.rem(order[d] + 2, n)
        reduce_copy(d, b, n - 2).wait_send()
        gather_copy(d, b, n - 2, c).wait()
    for d in range(2):
        update(d, lax.rem(order[d] + 2, n))


def emit_kernel(pieces, *refs):
    count = len(refs) // 2
    sources, targets, sem = refs[:count], refs[count:-1], refs[-1]
    size = sources[0].shape[0] // pieces
    copies = [
        pltpu.make_async_copy(
            sources[i].at[pl.ds(k * size, size)], targets[i].at[pl.ds(k * size, size)], sem.at[i, k]
        )
        for k in range(pieces) for i in range(count)
    ]
    for copy in copies:
        copy.start()
    for copy in copies:
        copy.wait()


def emit(arrays, pieces):
    return pl.pallas_call(
        functools.partial(emit_kernel, pieces),
        out_shape=tuple(jax.ShapeDtypeStruct(x.shape, x.dtype) for x in arrays),
        in_specs=[pl.BlockSpec(memory_space=pltpu.VMEM)] * len(arrays),
        out_specs=tuple(pl.BlockSpec(memory_space=pltpu.HBM) for _ in arrays),
        scratch_shapes=[pltpu.SemaphoreType.DMA((len(arrays), pieces))],
        compiler_params=pltpu.CompilerParams(vmem_limit_bytes=VMEM_LIMIT),
        name="emit",
    )(*arrays)


def body(slow_weights, fast_weights, momentum):
    n, m = lax.axis_size("dp"), lax.axis_size("mp")
    layers, depth, cols = slow_weights.shape
    rows = layers * depth
    max_norm = CLIP_LEVEL * math.sqrt(rows * cols * m)
    subs = SUBS
    while rows % (n * subs * 16):
        subs -= 1
    sub = rows // (n * subs)
    slow = slow_weights.reshape(rows, cols)
    hbm = pl.BlockSpec(memory_space=pltpu.HBM)
    vmem = pl.BlockSpec(memory_space=pltpu.VMEM)
    flat = (slow_weights, fast_weights, momentum)
    flat = [
        pltpu.with_memory_space_constraint(x.reshape(rows, cols), pltpu.HBM) for x in flat
    ]
    results = pl.pallas_call(
        functools.partial(kernel, n, m, subs, max_norm),
        out_shape=(
            jax.ShapeDtypeStruct((rows, cols), jnp.float32),
            jax.ShapeDtypeStruct((rows, cols), jnp.float32),
            jax.ShapeDtypeStruct((rows, cols), jnp.bfloat16),
        ),
        in_specs=[hbm, hbm, hbm],
        out_specs=(vmem, vmem, vmem),
        scratch_shapes=[
            pltpu.VMEM((2, subs, n, sub, cols // 2), jnp.float32),
            pltpu.VMEM((rows, cols), jnp.float32),
            pltpu.VMEM((rows, cols), jnp.bfloat16),
            pltpu.VMEM((rows, cols), jnp.float32),
            pltpu.VMEM((rows, cols), jnp.float32),
            pltpu.VMEM((n, 8, cols // 2), jnp.float32),
            pltpu.VMEM((m, 8, cols // 2), jnp.float32),
            pltpu.SemaphoreType.DMA,
            pltpu.SemaphoreType.DMA((2, 2, n)),
            pltpu.SemaphoreType.DMA((2, subs, 2 * n - 2)),
            pltpu.SemaphoreType.DMA((2, subs, 2 * n - 2)),
            pltpu.SemaphoreType.DMA((n,)),
            pltpu.SemaphoreType.DMA((n,)),
            pltpu.SemaphoreType.DMA((m,)),
            pltpu.SemaphoreType.DMA((m,)),
        ],
        compiler_params=pltpu.CompilerParams(
            collective_id=0, has_side_effects=True, vmem_limit_bytes=VMEM_LIMIT
        ),
        name="ring",
    )(*flat)
    slow_next, momentum_next, fast_next = emit(results, 4)
    return (
        slow_next.reshape(slow_weights.shape),
        momentum_next.reshape(slow_weights.shape),
        fast_next.reshape(fast_weights.shape),
    )


def solution(mesh):
    in_specs = (P(None, None, "mp"), P("dp", None, None, "mp"), P(None, None, "mp"))
    out_specs = (P(None, None, "mp"), P(None, None, "mp"), P("dp", None, None, "mp"))
    return jax.shard_map(body, mesh=mesh, in_specs=in_specs, out_specs=out_specs, check_vma=False)
```

```python
import functools
import math

import jax
import jax.numpy as jnp
from jax import lax
from jax.experimental import pallas as pl
from jax.experimental.pallas import tpu as pltpu
from jax.sharding import PartitionSpec as P

MOMENTUM_RATE = 0.9
OUTER_RATE = 0.7
CLIP_LEVEL = 0.2
EPSILON = 1e-06
MESH = pl.DeviceIdType.MESH
SUBS = 4
VMEM_LIMIT = 24 * 1024 * 1024


def device_at(place, n):
    half = n // 2
    up = 2 * place
    down = 2 * (n - 1 - place) + 1
    return jnp.where(place < half, up, down)


def kernel(n, m, subs, max_norm, slow_hbm, fast_hbm, moment_hbm,
           slow_out, moment_out, fast_out,
           ring, slow_ref, fast_ref, moment_ref, pseudo_ref, parts, norms, moment_sem, load_sem, send_sem, recv_sem,
           part_send, part_recv, norm_send, norm_recv):
    rows, cols = slow_ref.shape
    chunk = rows // n
    sub = chunk // subs
    half = cols // 2
    me = lax.axis_index("dp")
    mine = lax.axis_index("mp")
    z, y = me // 2, lax.rem(me, 2)
    place = jnp.where(y == 0, z, n - 1 - z)
    right = device_at(lax.rem(place + 1, n), n)
    left = device_at(lax.rem(place + n - 1, n), n)
    goal = (right, left)
    order = (place, lax.rem(n - place, n))

    def load(d, k):
        c = lax.rem(order[d] - k + n, n)
        at = (pl.ds(pl.multiple_of(c * chunk, chunk), chunk), pl.ds(d * half, half))
        return (
            pltpu.make_async_copy(slow_hbm.at[at], slow_ref.at[at], load_sem.at[0, d, k]),
            pltpu.make_async_copy(fast_hbm.at[at], fast_ref.at[at], load_sem.at[1, d, k]),
        )

    for d in range(2):
        for copy in load(d, 0):
            copy.start()
    barrier = pltpu.get_barrier_semaphore()
    for other in (left, right):
        pl.semaphore_signal(barrier, inc=1, device_id={"dp": other}, device_id_type=MESH)
    for k in range(1, m):
        pl.semaphore_signal(
            barrier, inc=1, device_id={"mp": lax.rem(mine + k, m)}, device_id_type=MESH
        )
    moment_load = pltpu.make_async_copy(moment_hbm, moment_ref, moment_sem)

    def start_row(c, b):
        return pl.multiple_of(c * chunk + b * sub, sub)

    def own(d, b, c):
        at = (pl.ds(start_row(c, b), sub), pl.ds(d * half, half))
        return slow_ref[at] - fast_ref[at].astype(jnp.float32)

    def reduce_copy(d, b, s):
        return pltpu.make_async_remote_copy(
            src_ref=ring.at[d, b, s], dst_ref=ring.at[d, b, s + 1],
            send_sem=send_sem.at[d, b, s], recv_sem=recv_sem.at[d, b, s],
            device_id={"dp": goal[d]}, device_id_type=MESH,
        )

    def gather_copy(d, b, s, c):
        at = (pl.ds(start_row(c, b), sub), pl.ds(d * half, half))
        return pltpu.make_async_remote_copy(
            src_ref=pseudo_ref.at[at], dst_ref=pseudo_ref.at[at],
            send_sem=send_sem.at[d, b, n - 1 + s], recv_sem=recv_sem.at[d, b, n - 1 + s],
            device_id={"dp": goal[d]}, device_id_type=MESH,
        )

    def part_copy(k):
        return pltpu.make_async_remote_copy(
            src_ref=parts.at[me], dst_ref=parts.at[me],
            send_sem=part_send.at[k], recv_sem=part_recv.at[k],
            device_id={"dp": lax.rem(me + k, n)}, device_id_type=MESH,
        )

    def norm_copy(k):
        return pltpu.make_async_remote_copy(
            src_ref=norms.at[mine], dst_ref=norms.at[mine],
            send_sem=norm_send.at[k], recv_sem=norm_recv.at[k],
            device_id={"mp": lax.rem(mine + k, m)}, device_id_type=MESH,
        )

    streams = [(d, b) for b in range(subs) for d in range(2)]
    for k in range(1, n):
        for d in range(2):
            for copy in load(d, k):
                copy.start()
    for d in range(2):
        for copy in load(d, 0):
            copy.wait()
    pl.semaphore_wait(barrier, 2 + m - 1)
    for d, b in streams:
        ring[d, b, 0] = own(d, b, order[d])
        reduce_copy(d, b, 0).start()
    moment_load.start()

    def reduce_step(s, carry):
        for d in range(2):
            for copy in load(d, s + 1):
                copy.wait()
        for d, b in streams:
            c = lax.rem(order[d] - s - 1 + n, n)
            reduce_copy(d, b, s).wait_recv()
            ring[d, b, s + 1] = ring[d, b, s + 1] + own(d, b, c)
            reduce_copy(d, b, s + 1).start()
        return carry

    lax.fori_loop(0, n - 2, reduce_step, 0)
    for d in range(2):
        for copy in load(d, n - 1):
            copy.wait()
    part = jnp.zeros((8, half), jnp.float32)
    for d, b in streams:
        c = lax.rem(order[d] + 1, n)
        reduce_copy(d, b, n - 2).wait_recv()
        value = (ring[d, b, n - 1] + own(d, b, c)) / n
        pseudo_ref[pl.ds(start_row(c, b), sub), pl.ds(d * half, half)] = value
        gather_copy(d, b, 0, c).start()
        part = part + jnp.sum((value * value).reshape(sub // 8, 8, half), axis=0)
    parts[me] = part

    def gather_step(s, carry):
        for d, b in streams:
            c = lax.rem(order[d] - s + n, n)
            gather_copy(d, b, s, c).wait_recv()
            gather_copy(d, b, s + 1, c).start()
        return carry

    second = (n - 2) // 2
    first = second // 2
    for k in range(1, n):
        part_copy(k).start()
    lax.fori_loop(0, first, gather_step, 0)
    for k in range(1, n):
        part_copy(k).wait_recv()
    norm = parts[0]
    for j in range(1, n):
        norm = norm + parts[j]
    norms[mine] = norm
    for k in range(1, m):
        norm_copy(k).start()
    lax.fori_loop(first, second, gather_step, 0)
    for k in range(1, m):
        norm_copy(k).wait_recv()
    total = norms[0]
    for j in range(1, m):
        total = total + norms[j]
    total = jnp.sum(jnp.sum(total, axis=1, keepdims=True), axis=0, keepdims=True)
    factor = jnp.minimum(1.0, max_norm / (jnp.sqrt(total) + EPSILON))
    moment_load.wait()

    def update(d, c, start=0, size=chunk):
        at = (pl.ds(pl.multiple_of(c * chunk + start, 16), size), pl.ds(d * half, half))
        gradient = factor * pseudo_ref[at]
        moment = MOMENTUM_RATE * moment_ref[at] + gradient
        slow = slow_ref[at] - OUTER_RATE * (gradient + MOMENTUM_RATE * moment)
        moment_out[at] = moment
        slow_out[at] = slow
        fast_out[at] = slow.astype(fast_out.dtype)

    def update_step(s, carry):
        gather_step(s, carry)
        for d in range(2):
            update(d, lax.rem(order[d] - s + n, n))
            update(d, lax.rem(order[d] - (s - second) + n, n))
        return carry

    lax.fori_loop(second, n - 2, update_step, 0)
    for d in range(2):
        update(d, lax.rem(order[d] + 1, n))
    for k in range(1, n):
        part_copy(k).wait_send()
    for k in range(1, m):
        norm_copy(k).wait_send()

    def drain(s, carry):
        for d, b in streams:
            reduce_copy(d, b, s).wait_send()
            gather_copy(d, b, s, 0).wait_send()
        return carry

    lax.fori_loop(0, n - 2, drain, 0)
    for d, b in streams:
        c = lax.rem(order[d] + 2, n)
        reduce_copy(d, b, n - 2).wait_send()
        gather_copy(d, b, n - 2, c).wait()
        update(d, c, b * sub, sub)


def emit_kernel(pieces, *refs):
    count = len(refs) // 2
    sources, targets, sem = refs[:count], refs[count:-1], refs[-1]
    size = sources[0].shape[0] // pieces
    copies = [
        pltpu.make_async_copy(
            sources[i].at[pl.ds(k * size, size)], targets[i].at[pl.ds(k * size, size)], sem.at[i, k]
        )
        for k in range(pieces) for i in range(count)
    ]
    for copy in copies:
        copy.start()
    for copy in copies:
        copy.wait()


def emit(arrays, pieces):
    return pl.pallas_call(
        functools.partial(emit_kernel, pieces),
        out_shape=tuple(jax.ShapeDtypeStruct(x.shape, x.dtype) for x in arrays),
        in_specs=[pl.BlockSpec(memory_space=pltpu.VMEM)] * len(arrays),
        out_specs=tuple(pl.BlockSpec(memory_space=pltpu.HBM) for _ in arrays),
        scratch_shapes=[pltpu.SemaphoreType.DMA((len(arrays), pieces))],
        compiler_params=pltpu.CompilerParams(vmem_limit_bytes=VMEM_LIMIT),
        name="emit",
    )(*arrays)


def body(slow_weights, fast_weights, momentum):
    n, m = lax.axis_size("dp"), lax.axis_size("mp")
    layers, depth, cols = slow_weights.shape
    rows = layers * depth
    max_norm = CLIP_LEVEL * math.sqrt(rows * cols * m)
    subs = SUBS
    while rows % (n * subs * 16):
        subs -= 1
    sub = rows // (n * subs)
    slow = slow_weights.reshape(rows, cols)
    hbm = pl.BlockSpec(memory_space=pltpu.HBM)
    vmem = pl.BlockSpec(memory_space=pltpu.VMEM)
    flat = (slow_weights, fast_weights, momentum)
    flat = [
        pltpu.with_memory_space_constraint(x.reshape(rows, cols), pltpu.HBM) for x in flat
    ]
    results = pl.pallas_call(
        functools.partial(kernel, n, m, subs, max_norm),
        out_shape=(
            jax.ShapeDtypeStruct((rows, cols), jnp.float32),
            jax.ShapeDtypeStruct((rows, cols), jnp.float32),
            jax.ShapeDtypeStruct((rows, cols), jnp.bfloat16),
        ),
        in_specs=[hbm, hbm, hbm],
        out_specs=(vmem, vmem, vmem),
        scratch_shapes=[
            pltpu.VMEM((2, subs, n, sub, cols // 2), jnp.float32),
            pltpu.VMEM((rows, cols), jnp.float32),
            pltpu.VMEM((rows, cols), jnp.bfloat16),
            pltpu.VMEM((rows, cols), jnp.float32),
            pltpu.VMEM((rows, cols), jnp.float32),
            pltpu.VMEM((n, 8, cols // 2), jnp.float32),
            pltpu.VMEM((m, 8, cols // 2), jnp.float32),
            pltpu.SemaphoreType.DMA,
            pltpu.SemaphoreType.DMA((2, 2, n)),
            pltpu.SemaphoreType.DMA((2, subs, 2 * n - 2)),
            pltpu.SemaphoreType.DMA((2, subs, 2 * n - 2)),
            pltpu.SemaphoreType.DMA((n,)),
            pltpu.SemaphoreType.DMA((n,)),
            pltpu.SemaphoreType.DMA((m,)),
            pltpu.SemaphoreType.DMA((m,)),
        ],
        compiler_params=pltpu.CompilerParams(
            collective_id=0, has_side_effects=True, vmem_limit_bytes=VMEM_LIMIT
        ),
        name="ring",
    )(*flat)
    slow_next, momentum_next, fast_next = emit(results, 4)
    return (
        slow_next.reshape(slow_weights.shape),
        momentum_next.reshape(slow_weights.shape),
        fast_next.reshape(fast_weights.shape),
    )


def solution(mesh):
    in_specs = (P(None, None, "mp"), P("dp", None, None, "mp"), P(None, None, "mp"))
    out_specs = (P(None, None, "mp"), P(None, None, "mp"), P("dp", None, None, "mp"))
    return jax.shard_map(body, mesh=mesh, in_specs=in_specs, out_specs=out_specs, check_vma=False)
```
